32 devices in a mesh: fsdp: 32 (over z, y, x, core).
Axes of the slice: x: 2, y: 2, z: 4, core: 2. Of those that a mesh axis runs over, the one named last changes fastest.
Arguments:
- grads: bfloat16 [32, 20736, 128], P('fsdp'), may hold values from -15000 to 15000
- params: float32 [20736, 128], P('fsdp'), may hold values from -0.1875 to 0.1875
- moment: float32 [20736, 128], P('fsdp'), may hold values from -6 to 6
- second: float32 [20736, 128], P('fsdp'), may hold values from 0.1 to 4
- teacher: float32 [20736, 128], P('fsdp'), may hold values from -0.1875 to 0.1875
Outputs:
- params_out: float32 [20736, 128], P('fsdp')
- moment_out: float32 [20736, 128], P('fsdp')
- second_out: float32 [20736, 128], P('fsdp')
- teacher_out: float32 [20736, 128], P('fsdp')
- weights_out: bfloat16 [20736, 128], replicated
The draws below stay inside these ranges and needn't reach their ends.
All inputs are finite; a program needn't handle non-finite values.
Results may differ from the reference program's by a relative error of at most 0.001.
Values may be sent and summed in bfloat16 or wider, within the bound.
A program may use at most 128 MiB of HBM per device.

```python
import math
import jax
import jax.numpy as jnp
from jax import lax

D = 1152
ROWS = 20736
N_FSDP = 32


def draw_grads(key, part):
    keys = jax.random.split(jax.random.fold_in(key, 17), 6)
    positions = jnp.arange(ROWS, dtype=jnp.float32)
    rising = jnp.exp(jnp.log(3.0) * positions / ROWS)[:, None]
    row_spread = jnp.exp(jax.random.uniform(keys[0], (ROWS, 1), jnp.float32) * jnp.log(10.0))
    col_spread = jnp.exp(jax.random.uniform(keys[1], (1, 128), jnp.float32) * jnp.log(10.0))
    pairing = jax.random.permutation(keys[5], N_FSDP).astype(jnp.int32)
    block_of_row = (jnp.arange(ROWS, dtype=jnp.int32) // (ROWS // N_FSDP)).astype(jnp.int32)
    boost = jnp.where(block_of_row[None, :] == pairing[:, None], 8.0, 1.0).astype(jnp.float32)[:, :, None]
    noise = jnp.clip(jax.random.normal(keys[4], (N_FSDP, ROWS, 128), jnp.float32), -5.0, 5.0)
    return (noise * boost * rising * row_spread * col_spread).astype(jnp.bfloat16)


def level_of(stream_key, shape, cuts, low, top_value):
    level, own = 1.0, jax.random.fold_in(stream_key, 6)
    for dim, parts in cuts:
        steps = jnp.exp(jax.random.uniform(jax.random.fold_in(own, dim), (parts,), jnp.float32, low / len(cuts), top_value / len(cuts)))
        level = level * jnp.repeat(steps, shape[dim] // parts).reshape([-1 if axis == dim else 1 for axis in range(len(shape))])
    return level


def scatter_about(key, dims, scale, reach, pieces=(), held_as=jnp.bfloat16):
    loudness = level_of(key, dims, pieces, -0.22, 0.18) if pieces else 1.0
    values = jax.random.normal(key, dims, jnp.float32) * scale * loudness
    return jnp.minimum(jnp.maximum(values, -reach), reach).astype(held_as)


def setup_inputs(seed: int = 0) -> dict:
    key_of = jax.random.split(jax.random.key(seed), 6)
    return {
        "grads": draw_grads(jax.random.fold_in(key_of[5], 71), 0),
        "params": scatter_about(key_of[1], (ROWS, 128), D ** -0.5, 0.1875, ((0, 32),), jnp.float32),
        "moment": scatter_about(key_of[2], (ROWS, 128), 1.0, 6.0, ((0, 32),), jnp.float32),
        "second": jnp.clip(jnp.exp(math.log(4.0) - 3.6888794 * jax.random.uniform(key_of[3], (ROWS, 128), jnp.float32) ** level_of(key_of[3], (ROWS, 128), ((0, 32),), -0.2, 0.2)), 0.1, 4.0),
        "teacher": scatter_about(key_of[4], (ROWS, 128), D ** -0.5, 0.1875, ((0, 32),), jnp.float32),
    }


def reference(grads, params, moment, second, teacher):

    def accumulate(total, piece):
        return (total + piece.astype(jnp.float32), None)
    summed, _ = lax.scan(accumulate, jnp.zeros(grads.shape[1:], jnp.float32), grads)
    squares = jnp.sum(summed * summed)
    entries = grads.shape[1] * grads.shape[2]
    factor = 1.0 / jnp.sqrt(squares / jnp.float32(entries) + 1e-06)
    clipped = factor * summed
    moment_out = 0.9 * moment + 0.1 * clipped
    second_out = 0.95 * second + 0.05 * clipped * clipped
    first_fix = 1.0 - 0.9 ** 10
    second_fix = 1.0 - 0.95 ** 10
    update = moment_out / first_fix / (jnp.sqrt(second_out / second_fix) + 1e-08) + 0.1 * params
    params_out = params - 0.001 * update
    teacher_out = 0.9999 * teacher + 0.0001 * params_out
    weights_out = params_out.astype(jnp.bfloat16)
    return (params_out, moment_out, second_out, teacher_out, weights_out)
```

```python
import functools

import jax
import jax.numpy as jnp
from jax import lax
from jax.experimental import pallas as pl
from jax.experimental.pallas import tpu as pltpu
from jax.sharding import PartitionSpec as P

MESH = pl.DeviceIdType.MESH
SHARES = (0.395, 0.765)
VMEM_GRANT = 67000000
PIECES = 8
NARROW_SCALE = 2.0**12
NARROW_FLOOR = 2.0**-125


def adamw(factor, summed, params, moment, second, teacher):
    clipped = factor * summed
    moment_out = 0.9 * moment + 0.1 * clipped
    second_out = 0.95 * second + 0.05 * clipped * clipped
    first_fix = 1.0 - 0.9**10
    second_fix = 1.0 - 0.95**10
    update = moment_out / first_fix / (jnp.sqrt(second_out / second_fix) + 1e-08) + 0.1 * params
    params_out = params - 0.001 * update
    teacher_out = 0.9999 * teacher + 0.0001 * params_out
    return params_out, moment_out, second_out, teacher_out


def narrowed(v):
    v = v * NARROW_SCALE
    return (v * jnp.abs(v) * (v * v)).astype(jnp.bfloat16)


def widened(x):
    x = x.astype(jnp.float32)
    for _ in range(2):
        x = x * lax.rsqrt(jnp.maximum(jnp.abs(x), NARROW_FLOOR))
    return x * (1.0 / NARROW_SCALE)


def plain_body(grads, params, moment, second, teacher):
    summed = lax.psum_scatter(grads[0].astype(jnp.float32), "fsdp", scatter_dimension=0, tiled=True)
    squares = lax.psum(jnp.sum(summed * summed), "fsdp")
    entries = grads.shape[1] * grads.shape[2]
    factor = 1.0 / jnp.sqrt(squares / jnp.float32(entries) + 1e-06)
    outs = adamw(factor, summed, params, moment, second, teacher)
    weights_out = lax.all_gather(outs[0].astype(jnp.bfloat16), "fsdp", axis=0, tiled=True)
    return (*outs, weights_out)


def span(masks):
    held = [0]
    for mask in masks:
        held = held + [j | mask for j in held]
    return held


def kernel(
    n, entries, parts, orders,
    grads, params, moment, second, teacher,
    params_out, moment_out, second_out, teacher_out, weights,
    state, loc, peer, *rest,
):
    n_parts = len(parts)
    sends, recvs, gathered = rest[:n_parts], rest[n_parts : 2 * n_parts], rest[2 * n_parts : 3 * n_parts]
    (total, square, squares,
     state_sem, loc_sem, peer_send, peer_recv, rs_send, rs_recv,
     sq_send, sq_recv, ag_send, ag_recv, fw_send, fw_recv, out_sem) = rest[3 * n_parts :]
    half = n // 2
    bits = n.bit_length() - 1
    me = lax.axis_index("fsdp")
    steps = [(1 << i) * (1 - 2 * ((me // (1 << i)) % 2)) for i in range(bits)]

    def at(j):
        where = me
        for i in range(bits):
            if j >> i & 1:
                where = where + steps[i]
        return where

    def remote(src, dst, send, recv, j):
        return pltpu.make_async_remote_copy(
            src_ref=src, dst_ref=dst, send_sem=send, recv_sem=recv,
            device_id=(at(j),), device_id_type=MESH,
        )

    by_need = sorted(range(half), key=lambda j: -(j & 7).bit_count() * half - j)
    peer_copies, loc_copies = {}, {}
    for j in by_need:
        peer_copies[j] = remote(grads.at[at(2 * j + 1)], peer.at[j], peer_send.at[j], peer_recv.at[j], 1)
        peer_copies[j].start()
    for j in by_need:
        loc_copies[j] = pltpu.make_async_copy(grads.at[at(2 * j)], loc.at[j], loc_sem.at[j])
        loc_copies[j].start()

    ready = set()
    rs_copies = {}

    def value(p, j, stage):
        if j not in ready:
            ready.add(j)
            loc_copies[j].wait()
            peer_copies[j].wait_recv()
        rows = pl.ds(*parts[p])
        v = loc[j, rows, :].astype(jnp.float32) + peer[j, rows, :].astype(jnp.float32)
        for mask in orders[p][:stage]:
            rs_copies[p, j | mask].wait_recv()
            v = v + widened(recvs[p][j | mask])
        return v

    state_copies = [
        pltpu.make_async_copy(ref, state.at[i], state_sem.at[i])
        for i, ref in enumerate((params, moment, second, teacher))
    ]
    for copy in state_copies:
        copy.start()

    stages = bits - 1
    for stage in range(stages):
        todo = []
        for p in range(n_parts):
            mask, later = orders[p][stage], orders[p][stage + 1 :]
            todo.append([j | mask for j in reversed(span(later[::-1]))])
        for i in range(len(todo[0])):
            for p in range(n_parts):
                j, mask = todo[p][i], orders[p][stage]
                source, target = sends[p], recvs[p]
                source[j] = narrowed(value(p, j, stage))
                rs_copies[p, j] = remote(
                    source.at[j], target.at[j], rs_send.at[p, j], rs_recv.at[p, j], 2 * mask
                )
                rs_copies[p, j].start()

    acc = jnp.zeros(square.shape, jnp.float32)
    for p in range(n_parts):
        v = value(p, 0, stages)
        total[pl.ds(*parts[p]), :] = v
        acc = acc + jnp.sum((v * v).reshape(-1, *square.shape), axis=0)
    square[...] = acc

    def square_copy(k):
        return pltpu.make_async_remote_copy(
            src_ref=square, dst_ref=squares.at[k], send_sem=sq_send.at[k], recv_sem=sq_recv.at[k],
            device_id=(lax.rem(me + k, n),), device_id_type=MESH,
        )

    @pl.loop(1, n)
    def _(k):
        square_copy(k).start()

    @pl.loop(1, n)
    def _(k):
        square_copy(k).wait()

    all_squares = square[...] + jnp.sum(squares[1:], axis=0)
    all_squares = jnp.sum(jnp.sum(all_squares, axis=0, keepdims=True), axis=1, keepdims=True)
    all_squares = jnp.broadcast_to(all_squares, (1, square.shape[1]))
    factor = 1.0 / jnp.sqrt(all_squares / jnp.float32(entries) + 1e-06)

    ag_copies, fw_copies, out_copies = {}, {}, {}

    def forward(p, j, stage):
        mask = orders[p][::-1][stage]
        ag_copies[p, j | mask] = remote(
            gathered[p].at[j], gathered[p].at[j | mask],
            ag_send.at[p, j | mask], ag_recv.at[p, j | mask], 2 * mask,
        )
        ag_copies[p, j | mask].start()

    def settle(p, j):
        rows = pl.ds(*parts[p])
        place = weights.at[at(2 * j), rows]
        fw_copies[p, j] = remote(gathered[p].at[j], place, fw_send.at[p, j], fw_recv.at[p, j], 1)
        fw_copies[p, j].start()
        out_copies[p, j] = pltpu.make_async_copy(gathered[p].at[j], place, out_sem.at[p, j])
        out_copies[p, j].start()

    for copy in state_copies:
        copy.wait()
    for p in range(n_parts):
        rows = pl.ds(*parts[p])
        outs = adamw(factor, total[rows, :], *(state[i, rows, :] for i in range(4)))
        gathered[p][0] = outs[0].astype(jnp.bfloat16)
        forward(p, 0, 0)
        params_out[rows, :], moment_out[rows, :], second_out[rows, :], teacher_out[rows, :] = outs
    for stage in range(1, stages):
        for p in range(n_parts):
            forward(p, 0, stage)
    for p in range(n_parts):
        settle(p, 0)
    for stage in range(stages):
        for i in range(1 << stage):
            for p in range(n_parts):
                order = orders[p][::-1]
                j = span(order[:stage])[i] | order[stage]
                ag_copies[p, j].wait_recv()
                for later in range(stage + 1, stages):
                    forward(p, j, later)
                settle(p, j)

    for copy in fw_copies.values():
        copy.wait()
    for copy in out_copies.values():
        copy.wait()
    for copies in (peer_copies, rs_copies, ag_copies):
        for copy in copies.values():
            copy.wait_send()


def land(*refs):
    sources, places, held, (in_sem, out_sem) = refs[:5], refs[5:10], refs[10:15], refs[15:]
    jobs = [(i, pl.ds(0, sources[i].shape[0])) for i in range(4)]
    size = sources[4].shape[0] // PIECES // 16 * 16
    for k in range(PIECES):
        jobs.append((4, pl.ds(k * size, size if k < PIECES - 1 else sources[4].shape[0] - k * size)))
    jobs = jobs[4:] + jobs[:4]
    incoming = [
        pltpu.make_async_copy(sources[i].at[rows], held[i].at[rows], in_sem.at[k])
        for k, (i, rows) in enumerate(jobs)
    ]
    outgoing = [
        pltpu.make_async_copy(held[i].at[rows], places[i].at[rows], out_sem.at[k])
        for k, (i, rows) in enumerate(jobs)
    ]
    for copy in incoming:
        copy.start()
    for copy, out in zip(incoming, outgoing):
        copy.wait()
        out.start()
    for out in outgoing:
        out.wait()


def split(rows):
    first = int(rows * SHARES[0]) // 16 * 16
    second = int(rows * SHARES[1]) // 16 * 16
    return ((0, first), (first, second - first), (second, rows - second))


def fast_body(n, grads, params, moment, second, teacher):
    rows, lanes = params.shape
    half = n // 2
    parts = split(rows)
    masks = [1 << i for i in range(n.bit_length() - 2)]
    orders = (
        tuple(masks),
        (masks[1], masks[0], *masks[2:]),
        (*masks[2:], masks[0], masks[1]),
    )
    shard = jax.ShapeDtypeStruct((rows, lanes), jnp.float32)
    vmem, hbm, anywhere = (pl.BlockSpec(memory_space=space) for space in (pltpu.VMEM, pltpu.HBM, pl.ANY))
    narrow = [pltpu.VMEM((half, size, lanes), jnp.bfloat16) for _, size in parts]
    dma = pltpu.SemaphoreType.DMA
    per_part = dma((len(parts), half))
    outs = pl.pallas_call(
        functools.partial(kernel, n, grads.shape[1] * lanes, parts, orders),
        out_shape=(shard,) * 4 + (jax.ShapeDtypeStruct((n, rows, lanes), jnp.bfloat16),),
        in_specs=[anywhere] + [hbm] * 4,
        out_specs=(vmem,) * 4 + (anywhere,),
        scratch_shapes=[pltpu.VMEM((4, rows, lanes), jnp.float32)]
        + [pltpu.VMEM((half, rows, lanes), jnp.bfloat16)] * 2
        + narrow * 3
        + [
            pltpu.VMEM((rows, lanes), jnp.float32),
            pltpu.VMEM((8, lanes), jnp.float32),
            pltpu.VMEM((n, 8, lanes), jnp.float32),
            dma((4,)), dma((half,)), dma((half,)), dma((half,)),
            per_part, per_part,
            dma((n,)), dma((n,)),
            per_part, per_part, per_part, per_part, per_part,
        ],
        compiler_params=pltpu.CompilerParams(has_side_effects=True, vmem_limit_bytes=VMEM_GRANT),
    )(grads.reshape(n, rows, lanes), params, moment, second, teacher)
    shapes = (shard,) * 4 + (jax.ShapeDtypeStruct((n * rows, lanes), jnp.bfloat16),)
    return pl.pallas_call(
        land,
        out_shape=shapes,
        in_specs=[anywhere] * 5,
        out_specs=(anywhere,) * 5,
        scratch_shapes=[pltpu.VMEM(s.shape, s.dtype) for s in shapes] + [dma((4 + PIECES,))] * 2,
        compiler_params=pltpu.CompilerParams(vmem_limit_bytes=VMEM_GRANT),
    )(*outs[:4], outs[4].reshape(n * rows, lanes))


def body(n, grads, params, moment, second, teacher):
    if n & (n - 1) == 0 and 16 <= n <= 64 and params.shape[0] % 8 == 0 and params.shape[0] >= 128:
        return fast_body(n, grads, params, moment, second, teacher)
    return plain_body(grads, params, moment, second, teacher)


def solution(mesh):
    in_specs = (
        P("fsdp", None, None),
        P("fsdp", None),
        P("fsdp", None),
        P("fsdp", None),
        P("fsdp", None),
    )
    out_specs = (P("fsdp", None), P("fsdp", None), P("fsdp", None), P("fsdp", None), P())
    run = functools.partial(body, mesh.shape["fsdp"])
    return jax.shard_map(run, mesh=mesh, in_specs=in_specs, out_specs=out_specs, check_vma=False)
```

```python
import functools

import jax
import jax.numpy as jnp
from jax import lax
from jax.experimental import pallas as pl
from jax.experimental.pallas import tpu as pltpu
from jax.sharding import PartitionSpec as P

MESH = pl.DeviceIdType.MESH
SHARES = (0.395, 0.765)
VMEM_GRANT = 40000000
PIECES = 4
NARROW_SCALE = 2.0**12
NARROW_FLOOR = 2.0**-125


def adamw(factor, summed, params, moment, second, teacher):
    clipped = factor * summed
    moment_out = 0.9 * moment + 0.1 * clipped
    second_out = 0.95 * second + 0.05 * clipped * clipped
    first_fix = 1.0 - 0.9**10
    second_fix = 1.0 - 0.95**10
    update = moment_out / first_fix / (jnp.sqrt(second_out / second_fix) + 1e-08) + 0.1 * params
    params_out = params - 0.001 * update
    teacher_out = 0.9999 * teacher + 0.0001 * params_out
    return params_out, moment_out, second_out, teacher_out


def narrowed(v):
    v = v * NARROW_SCALE
    return (v * jnp.abs(v) * (v * v)).astype(jnp.bfloat16)


def widened(x):
    x = x.astype(jnp.float32)
    for _ in range(2):
        x = x * lax.rsqrt(jnp.maximum(jnp.abs(x), NARROW_FLOOR))
    return x * (1.0 / NARROW_SCALE)


def plain_body(grads, params, moment, second, teacher):
    summed = lax.psum_scatter(grads[0].astype(jnp.float32), "fsdp", scatter_dimension=0, tiled=True)
    squares = lax.psum(jnp.sum(summed * summed), "fsdp")
    entries = grads.shape[1] * grads.shape[2]
    factor = 1.0 / jnp.sqrt(squares / jnp.float32(entries) + 1e-06)
    outs = adamw(factor, summed, params, moment, second, teacher)
    weights_out = lax.all_gather(outs[0].astype(jnp.bfloat16), "fsdp", axis=0, tiled=True)
    return (*outs, weights_out)


def span(masks):
    held = [0]
    for mask in masks:
        held = held + [j | mask for j in held]
    return held


def kernel(
    n, entries, parts, orders,
    grads, params, moment, second, teacher,
    params_out, moment_out, second_out, teacher_out, weights,
    state, loc, peer, *rest,
):
    n_parts = len(parts)
    sends, recvs = rest[:n_parts], rest[n_parts : 2 * n_parts]
    (total, square, squares,
     state_sem, loc_sem, peer_send, peer_recv, rs_send, rs_recv,
     sq_send, sq_recv, ag_send, ag_recv, fw_send, fw_recv) = rest[2 * n_parts :]
    half = n // 2
    bits = n.bit_length() - 1
    me = lax.axis_index("fsdp")
    steps = [(1 << i) * (1 - 2 * ((me // (1 << i)) % 2)) for i in range(bits)]

    def at(j):
        where = me
        for i in range(bits):
            if j >> i & 1:
                where = where + steps[i]
        return where

    def remote(src, dst, send, recv, j):
        return pltpu.make_async_remote_copy(
            src_ref=src, dst_ref=dst, send_sem=send, recv_sem=recv,
            device_id=(at(j),), device_id_type=MESH,
        )

    barrier = pltpu.get_barrier_semaphore()
    for i in range(bits):
        pl.semaphore_signal(barrier, inc=1, device_id=(at(1 << i),), device_id_type=MESH)

    by_need = sorted(range(half), key=lambda j: -(j & 7).bit_count() * half - j)
    peer_copies, loc_copies = {}, {}
    for j in by_need:
        loc_copies[j] = pltpu.make_async_copy(grads.at[at(2 * j)], loc.at[j], loc_sem.at[j])
        loc_copies[j].start()
    pl.semaphore_wait(barrier, bits)
    for j in by_need:
        peer_copies[j] = remote(grads.at[at(2 * j + 1)], peer.at[j], peer_send.at[j], peer_recv.at[j], 1)
        peer_copies[j].start()

    ready = set()
    rs_copies = {}

    def value(p, j, stage):
        if j not in ready:
            ready.add(j)
            loc_copies[j].wait()
            peer_copies[j].wait_recv()
        rows = pl.ds(*parts[p])
        v = loc[j, rows, :].astype(jnp.float32) + peer[j, rows, :].astype(jnp.float32)
        for mask in orders[p][:stage]:
            rs_copies[p, j | mask].wait_recv()
            v = v + widened(recvs[p][j | mask])
        return v

    state_copies = [
        pltpu.make_async_copy(ref, state.at[i], state_sem.at[i])
        for i, ref in enumerate((params, moment, second, teacher))
    ]
    for copy in state_copies:
        copy.start()

    stages = bits - 1
    for stage in range(stages):
        todo = []
        for p in range(n_parts):
            mask, later = orders[p][stage], orders[p][stage + 1 :]
            todo.append([j | mask for j in reversed(span(later[::-1]))])
        for i in range(len(todo[0])):
            for p in range(n_parts):
                j, mask = todo[p][i], orders[p][stage]
                source, target = sends[p], recvs[p]
                source[j] = narrowed(value(p, j, stage))
                rs_copies[p, j] = remote(
                    source.at[j], target.at[j], rs_send.at[p, j], rs_recv.at[p, j], 2 * mask
                )
                rs_copies[p, j].start()

    acc = jnp.zeros(square.shape, jnp.float32)
    for p in range(n_parts):
        v = value(p, 0, stages)
        total[pl.ds(*parts[p]), :] = v
        acc = acc + jnp.sum((v * v).reshape(-1, *square.shape), axis=0)
    square[...] = acc

    def square_copy(k):
        return pltpu.make_async_remote_copy(
            src_ref=square, dst_ref=squares.at[k], send_sem=sq_send.at[k], recv_sem=sq_recv.at[k],
            device_id=(lax.rem(me + k, n),), device_id_type=MESH,
        )

    @pl.loop(1, n)
    def _(k):
        square_copy(k).start()

    @pl.loop(1, n)
    def _(k):
        square_copy(k).wait()

    all_squares = square[...] + jnp.sum(squares[1:], axis=0)
    all_squares = jnp.sum(jnp.sum(all_squares, axis=0, keepdims=True), axis=1, keepdims=True)
    all_squares = jnp.broadcast_to(all_squares, (1, square.shape[1]))
    factor = 1.0 / jnp.sqrt(all_squares / jnp.float32(entries) + 1e-06)

    ag_copies, fw_copies = {}, {}

    def place(p, j):
        return weights.at[at(2 * j), pl.ds(*parts[p])]

    def forward(p, j, stage):
        mask = orders[p][::-1][stage]
        ag_copies[p, j | mask] = remote(
            place(p, j), place(p, j), ag_send.at[p, j | mask], ag_recv.at[p, j | mask], 2 * mask
        )
        ag_copies[p, j | mask].start()

    def settle(p, j):
        fw_copies[p, j] = remote(place(p, j), place(p, j), fw_send.at[p, j], fw_recv.at[p, j], 1)
        fw_copies[p, j].start()

    for copy in state_copies:
        copy.wait()
    for p in range(n_parts):
        rows = pl.ds(*parts[p])
        outs = adamw(factor, total[rows, :], *(state[i, rows, :] for i in range(4)))
        weights[me, rows, :] = outs[0].astype(jnp.bfloat16)
        forward(p, 0, 0)
        params_out[rows, :], moment_out[rows, :], second_out[rows, :], teacher_out[rows, :] = outs
    for stage in range(1, stages):
        for p in range(n_parts):
            forward(p, 0, stage)
    for p in range(n_parts):
        settle(p, 0)
    for stage in range(stages):
        for i in range(1 << stage):
            for p in range(n_parts):
                order = orders[p][::-1]
                j = span(order[:stage])[i] | order[stage]
                ag_copies[p, j].wait_recv()
                for later in range(stage + 1, stages):
                    forward(p, j, later)
                settle(p, j)

    for copy in fw_copies.values():
        copy.wait()
    for copies in (peer_copies, rs_copies, ag_copies):
        for copy in copies.values():
            copy.wait_send()


def land(*refs):
    held, places, out_sem = refs[:5], refs[5:10], refs[10]
    size = held[4].shape[0] // PIECES // 16 * 16
    jobs = []
    for k in range(PIECES):
        jobs.append((4, pl.ds(k * size, size if k < PIECES - 1 else held[4].shape[0] - k * size)))
    jobs += [(i, pl.ds(0, held[i].shape[0])) for i in range(4)]
    outgoing = [
        pltpu.make_async_copy(held[i].at[rows], places[i].at[rows], out_sem.at[k])
        for k, (i, rows) in enumerate(jobs)
    ]
    for out in outgoing:
        out.start()
    for out in outgoing:
        out.wait()


def split(rows):
    first = int(rows * SHARES[0]) // 16 * 16
    second = int(rows * SHARES[1]) // 16 * 16
    return ((0, first), (first, second - first), (second, rows - second))


def fast_body(n, grads, params, moment, second, teacher):
    rows, lanes = params.shape
    half = n // 2
    parts = split(rows)
    masks = [1 << i for i in range(n.bit_length() - 2)]
    orders = (
        tuple(masks),
        (masks[1], masks[0], *masks[2:]),
        (*masks[2:], masks[0], masks[1]),
    )
    vmem, hbm = (pl.BlockSpec(memory_space=space) for space in (pltpu.VMEM, pltpu.HBM))
    narrow = [pltpu.VMEM((half, size, lanes), jnp.bfloat16) for _, size in parts]
    dma = pltpu.SemaphoreType.DMA
    per_part = dma((len(parts), half))
    outs = pl.pallas_call(
        functools.partial(kernel, n, grads.shape[1] * lanes, parts, orders),
        out_shape=(pltpu.VMEM((rows, lanes), jnp.float32),) * 4 + (pltpu.VMEM((n, rows, lanes), jnp.bfloat16),),
        in_specs=[hbm] * 5,
        out_specs=(vmem,) * 5,
        scratch_shapes=[pltpu.VMEM((4, rows, lanes), jnp.float32)]
        + [pltpu.VMEM((half, rows, lanes), jnp.bfloat16)] * 2
        + narrow * 2
        + [
            pltpu.VMEM((rows, lanes), jnp.float32),
            pltpu.VMEM((8, lanes), jnp.float32),
            pltpu.VMEM((n, 8, lanes), jnp.float32),
            dma((4,)), dma((half,)), dma((half,)), dma((half,)),
            per_part, per_part,
            dma((n,)), dma((n,)),
            per_part, per_part, per_part, per_part,
        ],
        compiler_params=pltpu.CompilerParams(
            collective_id=0, has_side_effects=True, vmem_limit_bytes=VMEM_GRANT
        ),
    )(*(pltpu.with_memory_space_constraint(x, pltpu.HBM) for x in (grads.reshape(n, rows, lanes), params, moment, second, teacher)))
    held = [pltpu.with_memory_space_constraint(x, pltpu.VMEM) for x in (*outs[:4], outs[4].reshape(n * rows, lanes))]
    return pl.pallas_call(
        land,
        out_shape=tuple(jax.ShapeDtypeStruct(x.shape, x.dtype) for x in held),
        in_specs=[vmem] * 5,
        out_specs=(hbm,) * 5,
        scratch_shapes=[dma((4 + PIECES,))],
        compiler_params=pltpu.CompilerParams(vmem_limit_bytes=VMEM_GRANT),
    )(*held)


def body(n, grads, params, moment, second, teacher):
    if n & (n - 1) == 0 and 16 <= n <= 64 and params.shape[0] % 8 == 0 and params.shape[0] >= 128:
        return fast_body(n, grads, params, moment, second, teacher)
    return plain_body(grads, params, moment, second, teacher)


def solution(mesh):
    in_specs = (
        P("fsdp", None, None),
        P("fsdp", None),
        P("fsdp", None),
        P("fsdp", None),
        P("fsdp", None),
    )
    out_specs = (P("fsdp", None), P("fsdp", None), P("fsdp", None), P("fsdp", None), P())
    run = functools.partial(body, mesh.shape["fsdp"])
    return jax.shard_map(run, mesh=mesh, in_specs=in_specs, out_specs=out_specs, check_vma=False)
```

```python
import functools

import jax
import jax.numpy as jnp
from jax import lax
from jax.experimental import pallas as pl
from jax.experimental.pallas import tpu as pltpu
from jax.sharding import PartitionSpec as P

MESH = pl.DeviceIdType.MESH
PLAN = (
    ("01z", 0.195), ("10z", 0.195), ("z01", 0.11),
    ("01z", 0.195), ("10z", 0.195), ("z10", 0.11),
)
VMEM_GRANT = 40000000
PIECES = 4
RS_WEIGHTS = (1.0, 1.0, 1.3, 1.8, 1.0)
AG_WEIGHTS = (1.0, 1.0, 1.0, 1.0, 1.0)
NARROW_SCALE = 2.0**12
NARROW_FLOOR = 2.0**-125


def adamw(factor, summed, params, moment, second, teacher):
    clipped = factor * summed
    moment_out = 0.9 * moment + 0.1 * clipped
    second_out = 0.95 * second + 0.05 * clipped * clipped
    first_fix = 1.0 - 0.9**10
    second_fix = 1.0 - 0.95**10
    update = moment_out / first_fix / (jnp.sqrt(second_out / second_fix) + 1e-08) + 0.1 * params
    params_out = params - 0.001 * update
    teacher_out = 0.9999 * teacher + 0.0001 * params_out
    return params_out, moment_out, second_out, teacher_out


def narrowed(v):
    v = v * NARROW_SCALE
    return (v * jnp.abs(v) * (v * v)).astype(jnp.bfloat16)


def widened(x):
    x = x.astype(jnp.float32)
    for _ in range(2):
        x = x * lax.rsqrt(jnp.maximum(jnp.abs(x), NARROW_FLOOR))
    return x * (1.0 / NARROW_SCALE)


def plain_body(grads, params, moment, second, teacher):
    summed = lax.psum_scatter(grads[0].astype(jnp.float32), "fsdp", scatter_dimension=0, tiled=True)
    squares = lax.psum(jnp.sum(summed * summed), "fsdp")
    entries = grads.shape[1] * grads.shape[2]
    factor = 1.0 / jnp.sqrt(squares / jnp.float32(entries) + 1e-06)
    outs = adamw(factor, summed, params, moment, second, teacher)
    weights_out = lax.all_gather(outs[0].astype(jnp.bfloat16), "fsdp", axis=0, tiled=True)
    return (*outs, weights_out)


def first_of(order, j):
    return next(i for i, mask in enumerate(order) if j & mask)


def kernel(
    n, entries, parts, orders,
    grads, params, moment, second, teacher,
    params_out, moment_out, second_out, teacher_out, weights,
    state, pairs, *rest,
):
    n_parts = len(parts)
    sends, recvs = rest[:n_parts], rest[n_parts : 2 * n_parts]
    (total, square, squares,
     state_sem, pair_sem, recv_sem, peer_send, rs_send, ag_send, fw_send, fw_recv,
     sq_send, sq_recv) = rest[2 * n_parts :]
    half = n // 2
    bits = n.bit_length() - 1
    me = lax.axis_index("fsdp")
    steps = [(1 << i) * (1 - 2 * ((me // (1 << i)) % 2)) for i in range(bits)]

    def at(j):
        where = me
        for i in range(bits):
            if j >> i & 1:
                where = where + steps[i]
        return where

    def remote(src, dst, send, recv, j):
        pltpu.make_async_remote_copy(
            src_ref=src, dst_ref=dst, send_sem=send, recv_sem=recv,
            device_id=(at(j),), device_id_type=MESH,
        ).start()

    def settled(ref, sem):
        pltpu.make_async_copy(ref, ref, sem).wait()

    barrier = pltpu.get_barrier_semaphore()
    for i in range(bits):
        pl.semaphore_signal(barrier, inc=1, device_id=(at(1 << i),), device_id_type=MESH)

    by_need = sorted(range(half), key=lambda j: (-j.bit_count(), -j))
    for j in by_need:
        pltpu.make_async_copy(grads.at[at(2 * j)], pairs.at[j, 0], pair_sem.at[j]).start()
    for i, ref in enumerate((params, moment, second, teacher)):
        pltpu.make_async_copy(ref, state.at[i], state_sem).start()
    pl.semaphore_wait(barrier, bits)
    for j in by_need:
        remote(grads.at[at(2 * j + 1)], pairs.at[j, 1], peer_send, pair_sem.at[j], 1)

    ready = set()

    def value(p, j, stage):
        if j not in ready:
            ready.add(j)
            settled(pairs.at[j], pair_sem.at[j])
        rows = pl.ds(*parts[p])
        v = pairs[j, 0, rows, :].astype(jnp.float32) + pairs[j, 1, rows, :].astype(jnp.float32)
        for mask in orders[p][:stage]:
            settled(recvs[p].at[j | mask], recv_sem.at[p, j | mask])
            v = v + widened(recvs[p][j | mask])
        return v

    def haul(weigh, j):
        return sum(weigh[i] for i in range(half.bit_length()) if j >> i & 1)

    def rs_key(t):
        return -haul(RS_WEIGHTS, t[1]), t[2], -t[1], t[0]

    def ag_key(t):
        return haul(AG_WEIGHTS, t[1]), -t[2], t[1], t[0]

    stages = bits - 1
    todo = [(p, j, first_of(orders[p], j)) for p in range(n_parts) for j in range(1, half)]
    for p, j, stage in sorted(todo, key=rs_key):
        sends[p][j] = narrowed(value(p, j, stage))
        remote(sends[p].at[j], recvs[p].at[j], rs_send, recv_sem.at[p, j], 2 * orders[p][stage])

    acc = jnp.zeros((8, square.shape[1]), jnp.float32)
    for p in range(n_parts):
        v = value(p, 0, stages)
        total[pl.ds(*parts[p]), :] = v
        acc = acc + jnp.sum((v * v).reshape(-1, *acc.shape), axis=0)
    square[...] = jnp.sum(acc, axis=0, keepdims=True)

    @pl.loop(1, n)
    def _(k):
        pltpu.make_async_remote_copy(
            src_ref=square, dst_ref=squares.at[k], send_sem=sq_send, recv_sem=sq_recv,
            device_id=(lax.rem(me + k, n),), device_id_type=MESH,
        ).start()

    settled(state, state_sem)
    settled(squares.at[1:], sq_recv)
    all_squares = square[...] + jnp.sum(squares[1:], axis=0)
    all_squares = jnp.sum(all_squares, axis=1, keepdims=True)
    all_squares = jnp.broadcast_to(all_squares, (1, square.shape[1]))
    factor = 1.0 / jnp.sqrt(all_squares / jnp.float32(entries) + 1e-06)

    def place(p, j):
        return weights.at[at(2 * j), pl.ds(*parts[p])]

    def onward(p, j):
        for mask in orders[p][: first_of(orders[p], j) if j else stages][::-1]:
            remote(place(p, j), place(p, j), ag_send, recv_sem.at[p, j | mask], 2 * mask)
        remote(place(p, j), place(p, j), fw_send, fw_recv, 1)

    for p in range(n_parts):
        rows = pl.ds(*parts[p])
        outs = adamw(factor, total[rows, :], *(state[i, rows, :] for i in range(4)))
        weights[me, rows, :] = outs[0].astype(jnp.bfloat16)
        onward(p, 0)
        params_out[rows, :], moment_out[rows, :], second_out[rows, :], teacher_out[rows, :] = outs
    for p, j, stage in sorted(todo, key=ag_key):
        settled(place(p, j), recv_sem.at[p, j])
        onward(p, j)

    settled(weights.at[:half], fw_recv)
    settled(weights.at[:half], fw_send)
    settled(weights.at[:half], peer_send)
    settled(weights.at[: half - 1], rs_send)
    settled(weights.at[: half - 1], ag_send)
    settled(squares.at[1:], sq_send)


def land(*refs):
    held, places, out_sem = refs[:5], refs[5:10], refs[10]
    size = held[4].shape[0] // PIECES // 16 * 16
    jobs = []
    for k in range(PIECES):
        jobs.append((4, pl.ds(k * size, size if k < PIECES - 1 else held[4].shape[0] - k * size)))
    jobs += [(i, pl.ds(0, held[i].shape[0])) for i in range(4)]
    outgoing = [
        pltpu.make_async_copy(held[i].at[rows], places[i].at[rows], out_sem.at[k])
        for k, (i, rows) in enumerate(jobs)
    ]
    for out in outgoing:
        out.start()
    for out in outgoing:
        out.wait()


def split(rows):
    ends, share = [0], 0.0
    for _, part in PLAN[:-1]:
        share += part
        ends.append(int(rows * share) // 16 * 16)
    return tuple((lo, hi - lo) for lo, hi in zip(ends, ends[1:] + [rows]))


def fast_body(n, grads, params, moment, second, teacher):
    rows, lanes = params.shape
    half = n // 2
    parts = split(rows)
    masks = [1 << i for i in range(n.bit_length() - 2)]
    axes = {"0": masks[:1], "1": masks[1:2], "z": masks[2:]}
    orders = tuple(tuple(mask for axis in plan for mask in axes[axis]) for plan, _ in PLAN)
    vmem, hbm = (pl.BlockSpec(memory_space=space) for space in (pltpu.VMEM, pltpu.HBM))
    narrow = [pltpu.VMEM((half, size, lanes), jnp.bfloat16) for _, size in parts]
    dma = pltpu.SemaphoreType.DMA
    outs = pl.pallas_call(
        functools.partial(kernel, n, grads.shape[1] * lanes, parts, orders),
        out_shape=(pltpu.VMEM((rows, lanes), jnp.float32),) * 4 + (pltpu.VMEM((n, rows, lanes), jnp.bfloat16),),
        in_specs=[hbm] * 5,
        out_specs=(vmem,) * 5,
        scratch_shapes=[pltpu.VMEM((4, rows, lanes), jnp.float32)]
        + [pltpu.VMEM((half, 2, rows, lanes), jnp.bfloat16)]
        + narrow * 2
        + [
            pltpu.VMEM((rows, lanes), jnp.float32),
            pltpu.VMEM((1, lanes), jnp.float32),
            pltpu.VMEM((n, 1, lanes), jnp.float32),
            dma, dma((half,)), dma((len(parts), half)), dma, dma, dma, dma, dma, dma, dma,
        ],
        compiler_params=pltpu.CompilerParams(
            collective_id=0, has_side_effects=True, vmem_limit_bytes=VMEM_GRANT
        ),
    )(*(pltpu.with_memory_space_constraint(x, pltpu.HBM) for x in (grads.reshape(n, rows, lanes), params, moment, second, teacher)))
    held = [pltpu.with_memory_space_constraint(x, pltpu.VMEM) for x in (*outs[:4], outs[4].reshape(n * rows, lanes))]
    return pl.pallas_call(
        land,
        out_shape=tuple(jax.ShapeDtypeStruct(x.shape, x.dtype) for x in held),
        in_specs=[vmem] * 5,
        out_specs=(hbm,) * 5,
        scratch_shapes=[dma((4 + PIECES,))],
        compiler_params=pltpu.CompilerParams(vmem_limit_bytes=VMEM_GRANT),
    )(*held)


def body(n, grads, params, moment, second, teacher):
    if n & (n - 1) == 0 and 16 <= n <= 64 and params.shape[0] % 8 == 0 and params.shape[0] >= 128:
        return fast_body(n, grads, params, moment, second, teacher)
    return plain_body(grads, params, moment, second, teacher)


def solution(mesh):
    in_specs = (
        P("fsdp", None, None),
        P("fsdp", None),
        P("fsdp", None),
        P("fsdp", None),
        P("fsdp", None),
    )
    out_specs = (P("fsdp", None), P("fsdp", None), P("fsdp", None), P("fsdp", None), P())
    run = functools.partial(body, mesh.shape["fsdp"])
    return jax.shard_map(run, mesh=mesh, in_specs=in_specs, out_specs=out_specs, check_vma=False)
```

```python
import functools

import jax
import jax.numpy as jnp
from jax import lax
from jax.experimental import pallas as pl
from jax.experimental.pallas import tpu as pltpu
from jax.sharding import PartitionSpec as P

MESH = pl.DeviceIdType.MESH
PLAN = (
    ("01z", 0.1977), ("10z", 0.1977), ("z01", 0.099),
    ("01z", 0.1977), ("10z", 0.1977), ("z10", 0.1113),
)
VMEM_GRANT = 40000000
PIECES = 4
RS_WEIGHTS = (1.0, 1.0, 1.3, 1.8, 1.0)
AG_WEIGHTS = (1.0, 1.0, 1.0, 1.0, 1.0)
NARROW_SCALE = 2.0**12
NARROW_FLOOR = 2.0**-125
FAR_WEIGHTS = (1.0, 1.0, 1.0, 2.0, 2.0)
RS_ORDER = (
    (1, 15), (3, 15), (2, 15), (5, 14), (5, 13), (5, 15), (2, 13), (0, 15), (4, 15), (4, 11),
    (2, 12), (1, 14), (3, 11), (2, 7), (1, 11), (0, 11), (0, 9), (2, 11), (5, 5), (5, 7),
    (1, 7), (1, 13), (0, 7), (4, 7), (0, 13), (4, 13), (2, 4), (2, 14), (5, 11), (5, 12),
    (5, 6), (4, 10), (4, 14), (2, 9), (1, 10), (5, 4), (1, 9), (4, 9), (3, 13), (3, 7),
    (0, 5), (0, 14), (2, 3), (3, 14), (1, 3), (2, 8), (2, 5), (1, 12), (3, 3), (5, 8),
    (4, 6), (2, 6), (2, 10), (5, 9), (4, 12), (1, 5), (3, 5), (0, 6), (0, 10), (5, 10),
    (3, 10), (3, 9), (0, 12), (1, 6), (3, 12), (0, 3), (2, 1), (4, 3), (1, 8), (4, 8),
    (0, 4), (4, 5), (3, 6), (5, 3), (0, 1), (1, 2), (1, 1), (0, 8), (2, 2), (3, 2),
    (1, 4), (3, 1), (3, 8), (4, 1), (0, 2), (3, 4), (4, 2), (5, 2), (5, 1), (4, 4),
)
AG_ORDER = (
    (0, 2), (1, 1), (0, 4), (2, 2), (3, 2), (0, 8), (1, 4), (4, 1), (1, 2), (1, 8),
    (3, 8), (3, 4), (4, 8), (5, 1), (0, 6), (2, 1), (1, 3), (1, 10), (4, 4), (1, 9),
    (0, 12), (1, 12), (3, 9), (1, 6), (5, 2), (1, 5), (0, 1), (5, 3), (2, 3), (3, 12),
    (4, 12), (2, 5), (2, 8), (2, 10), (0, 7), (3, 3), (4, 3), (4, 6), (0, 10), (3, 1),
    (3, 10), (4, 5), (4, 9), (1, 13), (5, 9), (3, 6), (0, 13), (2, 9), (1, 11), (0, 14),
    (5, 10), (3, 14), (5, 4), (5, 8), (4, 2), (5, 7), (5, 11), (3, 5), (5, 5), (2, 4),
    (4, 13), (2, 11), (0, 3), (2, 14), (4, 10), (1, 7), (0, 9), (3, 7), (5, 6), (2, 6),
    (0, 11), (3, 13), (0, 5), (4, 11), (4, 7), (5, 12), (5, 13), (1, 15), (2, 13), (5, 14),
    (4, 14), (2, 7), (2, 12), (5, 15), (1, 14), (3, 15), (3, 11), (4, 15), (0, 15), (2, 15),
)


def adamw(factor, summed, params, moment, second, teacher):
    clipped = factor * summed
    moment_out = 0.9 * moment + 0.1 * clipped
    second_out = 0.95 * second + 0.05 * clipped * clipped
    first_fix = 1.0 - 0.9**10
    second_fix = 1.0 - 0.95**10
    update = moment_out / first_fix / (jnp.sqrt(second_out / second_fix) + 1e-08) + 0.1 * params
    params_out = params - 0.001 * update
    teacher_out = 0.9999 * teacher + 0.0001 * params_out
    return params_out, moment_out, second_out, teacher_out


def narrowed(v):
    v = v * NARROW_SCALE
    return (v * jnp.abs(v) * (v * v)).astype(jnp.bfloat16)


def widened(x):
    x = x.astype(jnp.float32)
    for _ in range(2):
        x = x * lax.rsqrt(jnp.maximum(jnp.abs(x), NARROW_FLOOR))
    return x * (1.0 / NARROW_SCALE)


def plain_body(grads, params, moment, second, teacher):
    summed = lax.psum_scatter(grads[0].astype(jnp.float32), "fsdp", scatter_dimension=0, tiled=True)
    squares = lax.psum(jnp.sum(summed * summed), "fsdp")
    entries = grads.shape[1] * grads.shape[2]
    factor = 1.0 / jnp.sqrt(squares / jnp.float32(entries) + 1e-06)
    outs = adamw(factor, summed, params, moment, second, teacher)
    weights_out = lax.all_gather(outs[0].astype(jnp.bfloat16), "fsdp", axis=0, tiled=True)
    return (*outs, weights_out)


def first_of(order, j):
    return next(i for i, mask in enumerate(order) if j & mask)


def kernel(
    n, entries, parts, orders,
    grads, params, moment, second, teacher,
    params_out, moment_out, second_out, teacher_out, weights,
    state, pairs, *rest,
):
    n_parts = len(parts)
    sends, recvs = rest[:n_parts], rest[n_parts : 2 * n_parts]
    (total, square, squares,
     state_sem, pair_sem, recv_sem, peer_send, rs_send, ag_send, fw_send, fw_recv,
     sq_send, sq_recv) = rest[2 * n_parts :]
    half = n // 2
    bits = n.bit_length() - 1
    me = lax.axis_index("fsdp")
    steps = [(1 << i) * (1 - 2 * ((me // (1 << i)) % 2)) for i in range(bits)]

    def at(j):
        where = me
        for i in range(bits):
            if j >> i & 1:
                where = where + steps[i]
        return where

    def remote(src, dst, send, recv, j):
        pltpu.make_async_remote_copy(
            src_ref=src, dst_ref=dst, send_sem=send, recv_sem=recv,
            device_id=(at(j),), device_id_type=MESH,
        ).start()

    def settled(ref, sem):
        pltpu.make_async_copy(ref, ref, sem).wait()

    barrier = pltpu.get_barrier_semaphore()
    for i in range(bits):
        pl.semaphore_signal(barrier, inc=1, device_id=(at(1 << i),), device_id_type=MESH)

    by_need = sorted(range(half), key=lambda j: (-j.bit_count(), -j))
    for j in by_need:
        pltpu.make_async_copy(grads.at[at(2 * j)], pairs.at[j, 0], pair_sem.at[j]).start()
    for i, ref in enumerate((params, moment, second, teacher)):
        pltpu.make_async_copy(ref, state.at[i], state_sem).start()
    pl.semaphore_wait(barrier, bits)
    for j in by_need:
        remote(grads.at[at(2 * j + 1)], pairs.at[j, 1], peer_send, pair_sem.at[j], 1)

    ready = set()

    def value(p, j, stage):
        if j not in ready:
            ready.add(j)
            settled(pairs.at[j], pair_sem.at[j])
        rows = pl.ds(*parts[p])
        v = pairs[j, 0, rows, :].astype(jnp.float32) + pairs[j, 1, rows, :].astype(jnp.float32)
        for mask in orders[p][:stage]:
            settled(recvs[p].at[j | mask], recv_sem.at[p, j | mask])
            v = v + widened(recvs[p][j | mask])
        return v

    def haul(weigh, j):
        return sum(weigh[i] for i in range(half.bit_length()) if j >> i & 1)

    def rs_key(t):
        return -haul(RS_WEIGHTS, t[1]), t[2], -t[1], t[0]

    def ag_key(t):
        return haul(AG_WEIGHTS, t[1]), -t[2], t[1], t[0]

    def arranged(order, key):
        if len(order) != len(todo):
            return sorted(todo, key=key)
        return [(p, j, first_of(orders[p], j)) for p, j in order]

    stages = bits - 1
    todo = [(p, j, first_of(orders[p], j)) for p in range(n_parts) for j in range(1, half)]
    for p, j, stage in arranged(RS_ORDER, rs_key):
        sends[p][j] = narrowed(value(p, j, stage))
        remote(sends[p].at[j], recvs[p].at[j], rs_send, recv_sem.at[p, j], 2 * orders[p][stage])

    acc = jnp.zeros((8, square.shape[1]), jnp.float32)
    for p in range(n_parts):
        v = value(p, 0, stages)
        total[pl.ds(*parts[p]), :] = v
        acc = acc + jnp.sum((v * v).reshape(-1, *acc.shape), axis=0)
    square[...] = jnp.sum(acc, axis=0, keepdims=True)

    for k in sorted(range(1, n), key=lambda k: -haul(FAR_WEIGHTS, k >> 1) - (k & 1) / n):
        remote(square, squares.at[k], sq_send, sq_recv, k)

    settled(state, state_sem)
    settled(squares.at[1:], sq_recv)
    all_squares = square[...] + jnp.sum(squares[1:], axis=0)
    all_squares = jnp.sum(all_squares, axis=1, keepdims=True)
    all_squares = jnp.broadcast_to(all_squares, (1, square.shape[1]))
    factor = 1.0 / jnp.sqrt(all_squares / jnp.float32(entries) + 1e-06)

    def place(p, j):
        return weights.at[at(2 * j), pl.ds(*parts[p])]

    def onward(p, j):
        for mask in orders[p][: first_of(orders[p], j) if j else stages][::-1]:
            remote(place(p, j), place(p, j), ag_send, recv_sem.at[p, j | mask], 2 * mask)
        remote(place(p, j), place(p, j), fw_send, fw_recv, 1)

    for p in range(n_parts):
        rows = pl.ds(*parts[p])
        outs = adamw(factor, total[rows, :], *(state[i, rows, :] for i in range(4)))
        weights[me, rows, :] = outs[0].astype(jnp.bfloat16)
        onward(p, 0)
        params_out[rows, :], moment_out[rows, :], second_out[rows, :], teacher_out[rows, :] = outs
    for p, j, stage in arranged(AG_ORDER, ag_key):
        settled(place(p, j), recv_sem.at[p, j])
        onward(p, j)

    settled(weights.at[:half], fw_recv)
    settled(weights.at[:half], fw_send)
    settled(weights.at[:half], peer_send)
    settled(weights.at[: half - 1], rs_send)
    settled(weights.at[: half - 1], ag_send)
    settled(squares.at[1:], sq_send)


def land(*refs):
    held, places, out_sem = refs[:5], refs[5:10], refs[10]
    size = held[4].shape[0] // PIECES // 16 * 16
    jobs = []
    for k in range(PIECES):
        jobs.append((4, pl.ds(k * size, size if k < PIECES - 1 else held[4].shape[0] - k * size)))
    jobs += [(i, pl.ds(0, held[i].shape[0])) for i in range(4)]
    outgoing = [
        pltpu.make_async_copy(held[i].at[rows], places[i].at[rows], out_sem.at[k])
        for k, (i, rows) in enumerate(jobs)
    ]
    for out in outgoing:
        out.start()
    for out in outgoing:
        out.wait()


def split(rows):
    ends, share = [0], 0.0
    for _, part in PLAN[:-1]:
        share += part
        ends.append(int(rows * share) // 16 * 16)
    return tuple((lo, hi - lo) for lo, hi in zip(ends, ends[1:] + [rows]))


def fast_body(n, grads, params, moment, second, teacher):
    rows, lanes = params.shape
    half = n // 2
    parts = split(rows)
    masks = [1 << i for i in range(n.bit_length() - 2)]
    axes = {"0": masks[:1], "1": masks[1:2], "z": masks[2:]}
    orders = tuple(tuple(mask for axis in plan for mask in axes[axis]) for plan, _ in PLAN)
    vmem, hbm = (pl.BlockSpec(memory_space=space) for space in (pltpu.VMEM, pltpu.HBM))
    narrow = [pltpu.VMEM((half, size, lanes), jnp.bfloat16) for _, size in parts]
    dma = pltpu.SemaphoreType.DMA
    outs = pl.pallas_call(
        functools.partial(kernel, n, grads.shape[1] * lanes, parts, orders),
        out_shape=(pltpu.VMEM((rows, lanes), jnp.float32),) * 4 + (pltpu.VMEM((n, rows, lanes), jnp.bfloat16),),
        in_specs=[hbm] * 5,
        out_specs=(vmem,) * 5,
        scratch_shapes=[pltpu.VMEM((4, rows, lanes), jnp.float32)]
        + [pltpu.VMEM((half, 2, rows, lanes), jnp.bfloat16)]
        + narrow * 2
        + [
            pltpu.VMEM((rows, lanes), jnp.float32),
            pltpu.VMEM((1, lanes), jnp.float32),
            pltpu.VMEM((n, 1, lanes), jnp.float32),
            dma, dma((half,)), dma((len(parts), half)), dma, dma, dma, dma, dma, dma, dma,
        ],
        compiler_params=pltpu.CompilerParams(
            collective_id=0, has_side_effects=True, vmem_limit_bytes=VMEM_GRANT
        ),
    )(*(pltpu.with_memory_space_constraint(x, pltpu.HBM) for x in (grads.reshape(n, rows, lanes), params, moment, second, teacher)))
    held = [pltpu.with_memory_space_constraint(x, pltpu.VMEM) for x in (*outs[:4], outs[4].reshape(n * rows, lanes))]
    return pl.pallas_call(
        land,
        out_shape=tuple(jax.ShapeDtypeStruct(x.shape, x.dtype) for x in held),
        in_specs=[vmem] * 5,
        out_specs=(hbm,) * 5,
        scratch_shapes=[dma((4 + PIECES,))],
        compiler_params=pltpu.CompilerParams(vmem_limit_bytes=VMEM_GRANT),
    )(*held)


def body(n, grads, params, moment, second, teacher):
    if n & (n - 1) == 0 and 16 <= n <= 64 and params.shape[0] % 8 == 0 and params.shape[0] >= 128:
        return fast_body(n, grads, params, moment, second, teacher)
    return plain_body(grads, params, moment, second, teacher)


def solution(mesh):
    in_specs = (
        P("fsdp", None, None),
        P("fsdp", None),
        P("fsdp", None),
        P("fsdp", None),
        P("fsdp", None),
    )
    out_specs = (P("fsdp", None), P("fsdp", None), P("fsdp", None), P("fsdp", None), P())
    run = functools.partial(body, mesh.shape["fsdp"])
    return jax.shard_map(run, mesh=mesh, in_specs=in_specs, out_specs=out_specs, check_vma=False)
```

```python
import functools

import jax
import jax.numpy as jnp
from jax import lax
from jax.experimental import pallas as pl
from jax.experimental.pallas import tpu as pltpu
from jax.sharding import PartitionSpec as P

MESH = pl.DeviceIdType.MESH
PLAN = (
    ("01z", 0.2224), ("10z", 0.2224), ("z01", 0.099),
    ("01z", 0.173), ("10z", 0.173), ("z10", 0.1113),
)
VMEM_GRANT = 40000000
PIECES = 4
RS_WEIGHTS = (1.0, 1.0, 1.3, 1.8, 1.0)
AG_WEIGHTS = (1.0, 1.0, 1.0, 1.0, 1.0)
NARROW_SCALE = 2.0**12
NARROW_FLOOR = 2.0**-125
FAR_WEIGHTS = (1.0, 1.0, 1.0, 2.0, 2.0)
RS_ORDER = (
    (2, 15), (0, 15), (4, 15), (1, 15), (2, 14), (4, 14), (5, 15), (0, 13), (5, 7), (3, 15),
    (0, 7), (0, 11), (5, 13), (5, 14), (2, 7), (1, 11), (2, 13), (4, 11), (5, 12), (2, 11),
    (1, 14), (4, 13), (2, 10), (3, 11), (5, 5), (5, 11), (0, 14), (1, 13), (2, 12), (5, 9),
    (4, 3), (3, 7), (2, 6), (1, 7), (3, 13), (4, 7), (5, 10), (4, 9), (2, 4), (3, 5),
    (4, 10), (2, 5), (3, 14), (4, 12), (5, 8), (0, 10), (0, 12), (0, 9), (2, 8), (1, 10),
    (1, 9), (2, 3), (2, 9), (3, 10), (1, 6), (3, 6), (1, 5), (0, 6), (1, 12), (0, 5),
    (5, 4), (3, 9), (4, 8), (3, 12), (0, 8), (5, 6), (0, 3), (3, 3), (4, 5), (1, 3),
    (4, 6), (1, 8), (5, 3), (0, 1), (1, 4), (3, 1), (2, 1), (1, 2), (4, 1), (2, 2),
    (4, 2), (3, 8), (3, 4), (0, 2), (0, 4), (1, 1), (3, 2), (4, 4), (5, 2), (5, 1),
)
AG_ORDER = (
    (1, 1), (0, 2), (0, 4), (0, 8), (1, 4), (3, 2), (4, 1), (1, 8), (3, 8), (5, 1),
    (3, 4), (3, 1), (4, 8), (5, 2), (2, 2), (0, 6), (2, 4), (4, 4), (1, 6), (0, 12),
    (0, 3), (1, 12), (2, 1), (3, 12), (5, 3), (4, 9), (0, 9), (0, 5), (3, 3), (1, 5),
    (4, 12), (5, 5), (2, 3), (1, 9), (4, 5), (1, 2), (3, 10), (0, 14), (2, 8), (5, 8),
    (0, 7), (3, 9), (4, 6), (0, 10), (5, 9), (1, 3), (1, 13), (3, 6), (2, 10), (2, 9),
    (5, 10), (2, 6), (1, 14), (4, 2), (0, 1), (3, 5), (5, 6), (5, 11), (3, 14), (4, 11),
    (3, 13), (4, 13), (5, 7), (2, 11), (2, 5), (1, 7), (4, 7), (5, 4), (0, 13), (5, 14),
    (3, 11), (5, 13), (0, 11), (5, 12), (2, 12), (2, 13), (1, 11), (1, 15), (2, 7), (1, 10),
    (2, 14), (0, 15), (3, 7), (4, 14), (4, 10), (5, 15), (4, 3), (3, 15), (4, 15), (2, 15),
)


def adamw(factor, summed, params, moment, second, teacher):
    clipped = factor * summed
    moment_out = 0.9 * moment + 0.1 * clipped
    second_out = 0.95 * second + 0.05 * clipped * clipped
    first_fix = 1.0 - 0.9**10
    second_fix = 1.0 - 0.95**10
    update = moment_out / first_fix / (jnp.sqrt(second_out / second_fix) + 1e-08) + 0.1 * params
    params_out = params - 0.001 * update
    teacher_out = 0.9999 * teacher + 0.0001 * params_out
    return params_out, moment_out, second_out, teacher_out


def narrowed(v):
    v = v * NARROW_SCALE
    return (v * jnp.abs(v) * (v * v)).astype(jnp.bfloat16)


def widened(x):
    x = x.astype(jnp.float32)
    for _ in range(2):
        x = x * lax.rsqrt(jnp.maximum(jnp.abs(x), NARROW_FLOOR))
    return x * (1.0 / NARROW_SCALE)


def plain_body(grads, params, moment, second, teacher):
    summed = lax.psum_scatter(grads[0].astype(jnp.float32), "fsdp", scatter_dimension=0, tiled=True)
    squares = lax.psum(jnp.sum(summed * summed), "fsdp")
    entries = grads.shape[1] * grads.shape[2]
    factor = 1.0 / jnp.sqrt(squares / jnp.float32(entries) + 1e-06)
    outs = adamw(factor, summed, params, moment, second, teacher)
    weights_out = lax.all_gather(outs[0].astype(jnp.bfloat16), "fsdp", axis=0, tiled=True)
    return (*outs, weights_out)


def first_of(order, j):
    return next(i for i, mask in enumerate(order) if j & mask)


def kernel(
    n, entries, parts, orders,
    grads, params, moment, second, teacher,
    params_out, moment_out, second_out, teacher_out, weights,
    state, pairs, *rest,
):
    n_parts = len(parts)
    sends, recvs = rest[:n_parts], rest[n_parts : 2 * n_parts]
    (total, square, squares,
     state_sem, pair_sem, recv_sem, peer_send, rs_send, ag_send, fw_send, fw_recv,
     sq_send, sq_recv) = rest[2 * n_parts :]
    half = n // 2
    bits = n.bit_length() - 1
    me = lax.axis_index("fsdp")
    steps = [(1 << i) * (1 - 2 * ((me // (1 << i)) % 2)) for i in range(bits)]

    def at(j):
        where = me
        for i in range(bits):
            if j >> i & 1:
                where = where + steps[i]
        return where

    def remote(src, dst, send, recv, j):
        pltpu.make_async_remote_copy(
            src_ref=src, dst_ref=dst, send_sem=send, recv_sem=recv,
            device_id=(at(j),), device_id_type=MESH,
        ).start()

    def settled(ref, sem):
        pltpu.make_async_copy(ref, ref, sem).wait()

    barrier = pltpu.get_barrier_semaphore()
    for i in range(bits):
        pl.semaphore_signal(barrier, inc=1, device_id=(at(1 << i),), device_id_type=MESH)

    by_need = sorted(range(half), key=lambda j: (-j.bit_count(), -j))
    for j in by_need:
        pltpu.make_async_copy(grads.at[at(2 * j)], pairs.at[j, 0], pair_sem.at[j]).start()
    for i, ref in enumerate((params, moment, second, teacher)):
        pltpu.make_async_copy(ref, state.at[i], state_sem).start()
    pl.semaphore_wait(barrier, bits)
    for j in by_need:
        remote(grads.at[at(2 * j + 1)], pairs.at[j, 1], peer_send, pair_sem.at[j], 1)

    def slot(p, j):
        return [k for k in range(half) if not k & orders[p][0]].index(j)

    ready = set()

    def value(p, j, stage):
        if j not in ready:
            ready.add(j)
            settled(pairs.at[j], pair_sem.at[j])
        rows = pl.ds(*parts[p])
        v = pairs[j, 0, rows, :].astype(jnp.float32) + pairs[j, 1, rows, :].astype(jnp.float32)
        if stage:
            settled(recvs[p].at[:stage], recv_sem.at[p, slot(p, j)])
        for mask in orders[p][:stage]:
            v = v + widened(recvs[p][j | mask])
        return v

    def haul(weigh, j):
        return sum(weigh[i] for i in range(half.bit_length()) if j >> i & 1)

    def rs_key(t):
        return -haul(RS_WEIGHTS, t[1]), t[2], -t[1], t[0]

    def ag_key(t):
        return haul(AG_WEIGHTS, t[1]), -t[2], t[1], t[0]

    def arranged(order, key):
        if len(order) != len(todo):
            return sorted(todo, key=key)
        return [(p, j, first_of(orders[p], j)) for p, j in order]

    stages = bits - 1
    todo = [(p, j, first_of(orders[p], j)) for p in range(n_parts) for j in range(1, half)]
    for p, j, stage in arranged(RS_ORDER, rs_key):
        sends[p][j] = narrowed(value(p, j, stage))
        mask = orders[p][stage]
        remote(sends[p].at[j], recvs[p].at[j], rs_send, recv_sem.at[p, slot(p, j ^ mask)], 2 * mask)

    acc = jnp.zeros((8, square.shape[1]), jnp.float32)
    for p in range(n_parts):
        v = value(p, 0, stages)
        total[pl.ds(*parts[p]), :] = v
        acc = acc + jnp.sum((v * v).reshape(-1, *acc.shape), axis=0)
    square[...] = jnp.sum(acc, axis=0, keepdims=True)

    for k in sorted(range(1, n), key=lambda k: -haul(FAR_WEIGHTS, k >> 1) - (k & 1) / n):
        remote(square, squares.at[k], sq_send, sq_recv, k)

    settled(state, state_sem)
    settled(squares.at[1:], sq_recv)
    all_squares = square[...] + jnp.sum(squares[1:], axis=0)
    all_squares = jnp.sum(all_squares, axis=1, keepdims=True)
    all_squares = jnp.broadcast_to(all_squares, (1, square.shape[1]))
    factor = 1.0 / jnp.sqrt(all_squares / jnp.float32(entries) + 1e-06)

    arrivals = arranged(AG_ORDER, ag_key)
    leaves = [[j for q, j, stage in arrivals if q == p and not stage] for p in range(n_parts)]

    def landing(p, j):
        if j not in leaves[p]:
            return recv_sem.at[p, slot(p, j)]
        pair = leaves[p].index(j) // 2
        return recv_sem.at[p, half // 2 - 1 + pair if pair else 0]

    def place(p, j):
        return weights.at[at(2 * j), pl.ds(*parts[p])]

    def onward(p, j):
        for mask in orders[p][: first_of(orders[p], j) if j else stages][::-1]:
            remote(place(p, j), place(p, j), ag_send, landing(p, j | mask), 2 * mask)
        remote(place(p, j), place(p, j), fw_send, fw_recv, 1)

    for p in range(n_parts):
        rows = pl.ds(*parts[p])
        outs = adamw(factor, total[rows, :], *(state[i, rows, :] for i in range(4)))
        weights[me, rows, :] = outs[0].astype(jnp.bfloat16)
        onward(p, 0)
        params_out[rows, :], moment_out[rows, :], second_out[rows, :], teacher_out[rows, :] = outs
    for p, j, stage in arrivals:
        if stage:
            settled(place(p, j), landing(p, j))
            onward(p, j)
        elif leaves[p].index(j) % 2:
            settled(recvs[p].at[:2], landing(p, j))
            onward(p, leaves[p][leaves[p].index(j) - 1])
            onward(p, j)

    settled(weights.at[:half], fw_recv)
    settled(weights.at[:half], fw_send)
    settled(weights.at[:half], peer_send)
    settled(weights.at[: half - 1], rs_send)
    settled(weights.at[: half - 1], ag_send)
    settled(squares.at[1:], sq_send)


def land(*refs):
    held, places, out_sem = refs[:5], refs[5:10], refs[10]
    size = held[4].shape[0] // PIECES // 16 * 16
    jobs = []
    for k in range(PIECES):
        jobs.append((4, pl.ds(k * size, size if k < PIECES - 1 else held[4].shape[0] - k * size)))
    jobs += [(i, pl.ds(0, held[i].shape[0])) for i in range(4)]
    outgoing = [
        pltpu.make_async_copy(held[i].at[rows], places[i].at[rows], out_sem.at[k])
        for k, (i, rows) in enumerate(jobs)
    ]
    for out in outgoing:
        out.start()
    for out in outgoing:
        out.wait()


def split(rows):
    ends, share = [0], 0.0
    for _, part in PLAN[:-1]:
        share += part
        ends.append(int(rows * share) // 16 * 16)
    return tuple((lo, hi - lo) for lo, hi in zip(ends, ends[1:] + [rows]))


def fast_body(n, grads, params, moment, second, teacher):
    rows, lanes = params.shape
    half = n // 2
    parts = split(rows)
    masks = [1 << i for i in range(n.bit_length() - 2)]
    axes = {"0": masks[:1], "1": masks[1:2], "z": masks[2:]}
    orders = tuple(tuple(mask for axis in plan for mask in axes[axis]) for plan, _ in PLAN)
    vmem, hbm = (pl.BlockSpec(memory_space=space) for space in (pltpu.VMEM, pltpu.HBM))
    narrow = [pltpu.VMEM((half, size, lanes), jnp.bfloat16) for _, size in parts]
    dma = pltpu.SemaphoreType.DMA
    outs = pl.pallas_call(
        functools.partial(kernel, n, grads.shape[1] * lanes, parts, orders),
        out_shape=(pltpu.VMEM((rows, lanes), jnp.float32),) * 4 + (pltpu.VMEM((n, rows, lanes), jnp.bfloat16),),
        in_specs=[hbm] * 5,
        out_specs=(vmem,) * 5,
        scratch_shapes=[pltpu.VMEM((4, rows, lanes), jnp.float32)]
        + [pltpu.VMEM((half, 2, rows, lanes), jnp.bfloat16)]
        + narrow * 2
        + [
            pltpu.VMEM((rows, lanes), jnp.float32),
            pltpu.VMEM((1, lanes), jnp.float32),
            pltpu.VMEM((n, 1, lanes), jnp.float32),
            dma, dma((half,)), dma((len(parts), half // 2 + half // 4 - 1)), dma, dma, dma, dma, dma, dma, dma,
        ],
        compiler_params=pltpu.CompilerParams(
            collective_id=0, has_side_effects=True, vmem_limit_bytes=VMEM_GRANT
        ),
    )(*(pltpu.with_memory_space_constraint(x, pltpu.HBM) for x in (grads.reshape(n, rows, lanes), params, moment, second, teacher)))
    held = [pltpu.with_memory_space_constraint(x, pltpu.VMEM) for x in (*outs[:4], outs[4].reshape(n * rows, lanes))]
    return pl.pallas_call(
        land,
        out_shape=tuple(jax.ShapeDtypeStruct(x.shape, x.dtype) for x in held),
        in_specs=[vmem] * 5,
        out_specs=(hbm,) * 5,
        scratch_shapes=[dma((4 + PIECES,))],
        compiler_params=pltpu.CompilerParams(vmem_limit_bytes=VMEM_GRANT),
    )(*held)


def body(n, grads, params, moment, second, teacher):
    if n & (n - 1) == 0 and 16 <= n <= 64 and params.shape[0] % 8 == 0 and params.shape[0] >= 128:
        return fast_body(n, grads, params, moment, second, teacher)
    return plain_body(grads, params, moment, second, teacher)


def solution(mesh):
    in_specs = (
        P("fsdp", None, None),
        P("fsdp", None),
        P("fsdp", None),
        P("fsdp", None),
        P("fsdp", None),
    )
    out_specs = (P("fsdp", None), P("fsdp", None), P("fsdp", None), P("fsdp", None), P())
    run = functools.partial(body, mesh.shape["fsdp"])
    return jax.shard_map(run, mesh=mesh, in_specs=in_specs, out_specs=out_specs, check_vma=False)
```

```python
import functools

import jax
import jax.numpy as jnp
from jax import lax
from jax.experimental import pallas as pl
from jax.experimental.pallas import tpu as pltpu
from jax.sharding import PartitionSpec as P

MESH = pl.DeviceIdType.MESH
PLAN = (
    ("01z", 0.2224), ("10z", 0.2224), ("z01", 0.099),
    ("01z", 0.173), ("10z", 0.173), ("z10", 0.1113),
)
VMEM_GRANT = 40000000
PIECES = 4
RS_WEIGHTS = (1.0, 1.0, 1.3, 1.8, 1.0)
AG_WEIGHTS = (1.0, 1.0, 1.0, 1.0, 1.0)
NARROW_SCALE = 2.0**12
NARROW_FLOOR = 2.0**-125
FAR_WEIGHTS = (1.0, 1.0, 1.0, 2.0, 2.0)
RS_ORDER = (
    (2, 15), (0, 15), (4, 15), (1, 15), (2, 14), (4, 14), (5, 15), (0, 13), (5, 7), (3, 15),
    (0, 7), (0, 11), (5, 13), (5, 14), (2, 7), (1, 11), (2, 13), (4, 11), (5, 12), (2, 11),
    (1, 14), (4, 13), (2, 10), (3, 11), (5, 5), (5, 11), (0, 14), (1, 13), (2, 12), (5, 9),
    (4, 3), (3, 7), (2, 6), (1, 7), (3, 13), (4, 7), (5, 10), (4, 9), (2, 4), (3, 5),
    (4, 10), (2, 5), (3, 14), (4, 12), (5, 8), (0, 10), (0, 12), (0, 9), (2, 8), (1, 10),
    (1, 9), (2, 3), (2, 9), (3, 10), (1, 6), (3, 6), (1, 5), (0, 6), (1, 12), (0, 5),
    (5, 4), (3, 9), (4, 8), (3, 12), (0, 8), (5, 6), (0, 3), (3, 3), (4, 5), (1, 3),
    (4, 6), (1, 8), (5, 3), (0, 1), (1, 4), (3, 1), (2, 1), (1, 2), (4, 1), (2, 2),
    (4, 2), (3, 8), (3, 4), (0, 2), (0, 4), (1, 1), (3, 2), (4, 4), (5, 2), (5, 1),
)
AG_ORDER = (
    (1, 1), (0, 2), (0, 4), (0, 8), (1, 4), (3, 2), (4, 1), (1, 8), (3, 8), (5, 1),
    (3, 4), (3, 1), (4, 8), (5, 2), (2, 2), (0, 6), (2, 4), (4, 4), (1, 6), (0, 12),
    (0, 3), (1, 12), (2, 1), (3, 12), (5, 3), (4, 9), (0, 9), (0, 5), (3, 3), (1, 5),
    (4, 12), (5, 5), (2, 3), (1, 9), (4, 5), (1, 2), (3, 10), (0, 14), (2, 8), (5, 8),
    (0, 7), (3, 9), (4, 6), (0, 10), (5, 9), (1, 3), (1, 13), (3, 6), (2, 10), (2, 9),
    (5, 10), (2, 6), (1, 14), (4, 2), (0, 1), (3, 5), (5, 6), (5, 11), (3, 14), (4, 11),
    (3, 13), (4, 13), (5, 7), (2, 11), (2, 5), (1, 7), (4, 7), (5, 4), (0, 13), (5, 14),
    (3, 11), (5, 13), (0, 11), (5, 12), (2, 12), (2, 13), (1, 11), (1, 15), (2, 7), (1, 10),
    (2, 14), (0, 15), (3, 7), (4, 14), (4, 10), (5, 15), (4, 3), (3, 15), (4, 15), (2, 15),
)


def adamw(factor, summed, params, moment, second, teacher):
    clipped = factor * summed
    moment_out = 0.9 * moment + 0.1 * clipped
    second_out = 0.95 * second + 0.05 * clipped * clipped
    first_fix = 1.0 - 0.9**10
    second_fix = 1.0 - 0.95**10
    update = moment_out / first_fix / (jnp.sqrt(second_out / second_fix) + 1e-08) + 0.1 * params
    params_out = params - 0.001 * update
    teacher_out = 0.9999 * teacher + 0.0001 * params_out
    return params_out, moment_out, second_out, teacher_out


def narrowed(v):
    v = v * NARROW_SCALE
    return (v * jnp.abs(v) * (v * v)).astype(jnp.bfloat16)


def widened(x):
    x = x.astype(jnp.float32)
    for _ in range(2):
        x = x * lax.rsqrt(jnp.maximum(jnp.abs(x), NARROW_FLOOR))
    return x * (1.0 / NARROW_SCALE)


def plain_body(grads, params, moment, second, teacher):
    summed = lax.psum_scatter(grads[0].astype(jnp.float32), "fsdp", scatter_dimension=0, tiled=True)
    squares = lax.psum(jnp.sum(summed * summed), "fsdp")
    entries = grads.shape[1] * grads.shape[2]
    factor = 1.0 / jnp.sqrt(squares / jnp.float32(entries) + 1e-06)
    outs = adamw(factor, summed, params, moment, second, teacher)
    weights_out = lax.all_gather(outs[0].astype(jnp.bfloat16), "fsdp", axis=0, tiled=True)
    return (*outs, weights_out)


def first_of(order, j):
    return next(i for i, mask in enumerate(order) if j & mask)


def kernel(
    n, entries, parts, orders,
    grads, params, moment, second, teacher,
    params_out, moment_out, second_out, teacher_out, weights,
    state, pairs, *rest,
):
    n_parts = len(parts)
    sends, recvs = rest[:n_parts], rest[n_parts : 2 * n_parts]
    (total, square, squares,
     state_sem, pair_sem, recv_sem, peer_send, rs_send, ag_send, fw_send, fw_recv,
     sq_send, sq_recv, relay) = rest[2 * n_parts :]
    half = n // 2
    bits = n.bit_length() - 1
    me = lax.axis_index("fsdp")
    steps = [(1 << i) * (1 - 2 * ((me // (1 << i)) % 2)) for i in range(bits)]

    def at(j):
        where = me
        for i in range(bits):
            if j >> i & 1:
                where = where + steps[i]
        return where

    def remote(src, dst, send, recv, j):
        pltpu.make_async_remote_copy(
            src_ref=src, dst_ref=dst, send_sem=send, recv_sem=recv,
            device_id=(at(j),), device_id_type=MESH,
        ).start()

    def settled(ref, sem):
        pltpu.make_async_copy(ref, ref, sem).wait()

    barrier = pltpu.get_barrier_semaphore()
    lined = bits == 5
    greeted = [at(1 << i) for i in range(bits - lined)]
    inner = 0
    if lined:
        level = me // (n // 4)
        inner = (level + 1) // 2 % 2
        near = me + (3 - 2 * level) * (n // 4)

    def greet(sem, where):
        pl.semaphore_signal(sem, inc=1, device_id=(where,), device_id_type=MESH)

    for where in greeted:
        greet(barrier, where)
    if lined:
        pl.when(inner == 1)(lambda: greet(barrier, near))

    by_need = sorted(range(half), key=lambda j: (-j.bit_count(), -j))
    for j in by_need:
        pltpu.make_async_copy(grads.at[at(2 * j)], pairs.at[j, 0], pair_sem.at[j]).start()
    for i, ref in enumerate((params, moment, second, teacher)):
        pltpu.make_async_copy(ref, state.at[i], state_sem).start()
    pl.semaphore_wait(barrier, len(greeted) + inner)
    for j in by_need:
        remote(grads.at[at(2 * j + 1)], pairs.at[j, 1], peer_send, pair_sem.at[j], 1)

    def slot(p, j):
        return [k for k in range(half) if not k & orders[p][0]].index(j)

    ready, relayed = set(), []

    if lined:
        @pl.when(inner == 1)
        def _():
            greet(relay, greeted[-1])
            greet(relay, near)

    def value(p, j, stage):
        if j not in ready:
            ready.add(j)
            settled(pairs.at[j], pair_sem.at[j])
        rows = pl.ds(*parts[p])
        v = pairs[j, 0, rows, :].astype(jnp.float32) + pairs[j, 1, rows, :].astype(jnp.float32)
        if stage:
            settled(recvs[p].at[:stage], recv_sem.at[p, slot(p, j)])
        for mask in orders[p][:stage]:
            v = v + widened(recvs[p][j | mask])
        return v

    def haul(weigh, j):
        return sum(weigh[i] for i in range(half.bit_length()) if j >> i & 1)

    def rs_key(t):
        return -haul(RS_WEIGHTS, t[1]), t[2], -t[1], t[0]

    def ag_key(t):
        return haul(AG_WEIGHTS, t[1]), -t[2], t[1], t[0]

    def arranged(order, key):
        if len(order) != len(todo):
            return sorted(todo, key=key)
        return [(p, j, first_of(orders[p], j)) for p, j in order]

    stages = bits - 1
    todo = [(p, j, first_of(orders[p], j)) for p in range(n_parts) for j in range(1, half)]
    for p, j, stage in arranged(RS_ORDER, rs_key):
        sends[p][j] = narrowed(value(p, j, stage))
        if lined and orders[p][stage] == half // 2 and not relayed:
            relayed.append(True)
            pl.semaphore_wait(relay, 1)
        mask = orders[p][stage]
        remote(sends[p].at[j], recvs[p].at[j], rs_send, recv_sem.at[p, slot(p, j ^ mask)], 2 * mask)

    acc = jnp.zeros((8, square.shape[1]), jnp.float32)
    for p in range(n_parts):
        v = value(p, 0, stages)
        total[pl.ds(*parts[p]), :] = v
        acc = acc + jnp.sum((v * v).reshape(-1, *acc.shape), axis=0)
    square[...] = jnp.sum(acc, axis=0, keepdims=True)

    for k in sorted(range(1, n), key=lambda k: -haul(FAR_WEIGHTS, k >> 1) - (k & 1) / n):
        remote(square, squares.at[k], sq_send, sq_recv, k)

    settled(state, state_sem)
    settled(squares.at[1:], sq_recv)
    all_squares = square[...] + jnp.sum(squares[1:], axis=0)
    all_squares = jnp.sum(all_squares, axis=1, keepdims=True)
    all_squares = jnp.broadcast_to(all_squares, (1, square.shape[1]))
    factor = 1.0 / jnp.sqrt(all_squares / jnp.float32(entries) + 1e-06)

    arrivals = arranged(AG_ORDER, ag_key)
    leaves = [[j for q, j, stage in arrivals if q == p and not stage] for p in range(n_parts)]

    def landing(p, j):
        if j not in leaves[p]:
            return recv_sem.at[p, slot(p, j)]
        pair = leaves[p].index(j) // 2
        return recv_sem.at[p, half // 2 - 1 + pair if pair else 0]

    def place(p, j):
        return weights.at[at(2 * j), pl.ds(*parts[p])]

    def onward(p, j):
        for mask in orders[p][: first_of(orders[p], j) if j else stages][::-1]:
            remote(place(p, j), place(p, j), ag_send, landing(p, j | mask), 2 * mask)
        remote(place(p, j), place(p, j), fw_send, fw_recv, 1)

    for p in range(n_parts):
        rows = pl.ds(*parts[p])
        outs = adamw(factor, total[rows, :], *(state[i, rows, :] for i in range(4)))
        weights[me, rows, :] = outs[0].astype(jnp.bfloat16)
        onward(p, 0)
        params_out[rows, :], moment_out[rows, :], second_out[rows, :], teacher_out[rows, :] = outs
    for p, j, stage in arrivals:
        if stage:
            settled(place(p, j), landing(p, j))
            onward(p, j)
        elif leaves[p].index(j) % 2:
            settled(recvs[p].at[:2], landing(p, j))
            onward(p, leaves[p][leaves[p].index(j) - 1])
            onward(p, j)

    settled(weights.at[:half], fw_recv)
    settled(weights.at[:half], fw_send)
    settled(weights.at[:half], peer_send)
    settled(weights.at[: half - 1], rs_send)
    settled(weights.at[: half - 1], ag_send)
    settled(squares.at[1:], sq_send)


def land(*refs):
    held, places, out_sem = refs[:5], refs[5:10], refs[10]
    size = held[4].shape[0] // PIECES // 16 * 16
    jobs = []
    for k in range(PIECES):
        jobs.append((4, pl.ds(k * size, size if k < PIECES - 1 else held[4].shape[0] - k * size)))
    jobs += [(i, pl.ds(0, held[i].shape[0])) for i in range(4)]
    outgoing = [
        pltpu.make_async_copy(held[i].at[rows], places[i].at[rows], out_sem.at[k])
        for k, (i, rows) in enumerate(jobs)
    ]
    for out in outgoing:
        out.start()
    for out in outgoing:
        out.wait()


def split(rows):
    ends, share = [0], 0.0
    for _, part in PLAN[:-1]:
        share += part
        ends.append(int(rows * share) // 16 * 16)
    return tuple((lo, hi - lo) for lo, hi in zip(ends, ends[1:] + [rows]))


def fast_body(n, grads, params, moment, second, teacher):
    rows, lanes = params.shape
    half = n // 2
    parts = split(rows)
    masks = [1 << i for i in range(n.bit_length() - 2)]
    axes = {"0": masks[:1], "1": masks[1:2], "z": masks[2:]}
    orders = tuple(tuple(mask for axis in plan for mask in axes[axis]) for plan, _ in PLAN)
    vmem, hbm = (pl.BlockSpec(memory_space=space) for space in (pltpu.VMEM, pltpu.HBM))
    narrow = [pltpu.VMEM((half, size, lanes), jnp.bfloat16) for _, size in parts]
    dma = pltpu.SemaphoreType.DMA
    outs = pl.pallas_call(
        functools.partial(kernel, n, grads.shape[1] * lanes, parts, orders),
        out_shape=(pltpu.VMEM((rows, lanes), jnp.float32),) * 4 + (pltpu.VMEM((n, rows, lanes), jnp.bfloat16),),
        in_specs=[hbm] * 5,
        out_specs=(vmem,) * 5,
        scratch_shapes=[pltpu.VMEM((4, rows, lanes), jnp.float32)]
        + [pltpu.VMEM((half, 2, rows, lanes), jnp.bfloat16)]
        + narrow * 2
        + [
            pltpu.VMEM((rows, lanes), jnp.float32),
            pltpu.VMEM((1, lanes), jnp.float32),
            pltpu.VMEM((n, 1, lanes), jnp.float32),
            dma, dma((half,)), dma((len(parts), half // 2 + half // 4 - 1)), dma, dma, dma, dma, dma, dma, dma,
            pltpu.SemaphoreType.REGULAR,
        ],
        compiler_params=pltpu.CompilerParams(
            collective_id=0, has_side_effects=True, vmem_limit_bytes=VMEM_GRANT
        ),
    )(*(pltpu.with_memory_space_constraint(x, pltpu.HBM) for x in (grads.reshape(n, rows, lanes), params, moment, second, teacher)))
    held = [pltpu.with_memory_space_constraint(x, pltpu.VMEM) for x in (*outs[:4], outs[4].reshape(n * rows, lanes))]
    return pl.pallas_call(
        land,
        out_shape=tuple(jax.ShapeDtypeStruct(x.shape, x.dtype) for x in held),
        in_specs=[vmem] * 5,
        out_specs=(hbm,) * 5,
        scratch_shapes=[dma((4 + PIECES,))],
        compiler_params=pltpu.CompilerParams(vmem_limit_bytes=VMEM_GRANT),
    )(*held)


def body(n, grads, params, moment, second, teacher):
    if n & (n - 1) == 0 and 16 <= n <= 64 and params.shape[0] % 8 == 0 and params.shape[0] >= 128:
        return fast_body(n, grads, params, moment, second, teacher)
    return plain_body(grads, params, moment, second, teacher)


def solution(mesh):
    in_specs = (
        P("fsdp", None, None),
        P("fsdp", None),
        P("fsdp", None),
        P("fsdp", None),
        P("fsdp", None),
    )
    out_specs = (P("fsdp", None), P("fsdp", None), P("fsdp", None), P("fsdp", None), P())
    run = functools.partial(body, mesh.shape["fsdp"])
    return jax.shard_map(run, mesh=mesh, in_specs=in_specs, out_specs=out_specs, check_vma=False)
```
